256 devices in a mesh: seq: 16 (over z, core), head: 16 (over x, y).
Axes of the slice: x: 4, y: 4, z: 8, core: 2. Of those that a mesh axis runs over, the one named last changes fastest.
Arguments:
- queries: bfloat16 [8192, 4096], P('seq', 'head'), may hold values from -6 to 6
- keys: bfloat16 [8192, 1024], P(('seq', 'head')), may hold values from -6 to 6
- values: bfloat16 [8192, 1024], P(('seq', 'head')), may hold values from -3 to 3
- attn_out: bfloat16 [8192, 4096], P('seq', 'head'), may hold values from -1.796875 to 1.796875
- out_grad: bfloat16 [8192, 4096], P('seq', 'head'), may hold values from -6 to 6
- log_norm: float32 [32, 8192], P('head', 'seq'), may hold values from 3.5 to 5.5
- block_layout: int32 [32, 64, 64], P('head'), may hold values 0 or 1
- document_ids: int32 [8192], replicated, may hold values from 0 to 7, never falling along the last dimension, each value on 1 to 4096 neighbouring positions
- block_order: int32 [64], replicated, may hold values from 0 to 63, each once
Outputs:
- query_grad: float32 [8192, 4096], P('seq', 'head')
- key_grad: float32 [8192, 1024], P(('seq', 'head'))
- value_grad: float32 [8192, 1024], P(('seq', 'head'))
The draws below stay inside these ranges and needn't reach their ends.
Inputs may be any that keep to these rules, and one draw needn't show every extreme that they name: `document_ids`: never falls along the sequence position; each document covers 1 to 4096 positions, one exactly 4096. `block_order`: each sequence block once.
All inputs are finite; a program needn't handle non-finite values.
Results may differ from the reference program's by a relative error of at most 0.0029.
Values may be sent and summed in bfloat16 or wider, within the bound.
No kernel may reach another device: no remote copies, remote signals or barrier semaphores. Data moves between devices by JAX's collectives and lax.ppermute only.
A program may use at most 128 MiB of HBM per device.

```python
import math
import jax
import jax.numpy as jnp
import numpy as np
from jax import lax

D_HEAD = 128
GROUP = 4
BLOCK = 128
DOCS = 8
HEADS = 32
KV_HEADS = 8
SEQ = 8192
NBLK = 64


def touch_ends(entries, stream_key, low, largest):
    longest = entries.shape.index(max(entries.shape))
    spots = []
    for shift in (0, 1):
        where = [jax.random.randint(jax.random.fold_in(stream_key, axis), (), 0, length) for axis, length in enumerate(entries.shape)]
        where[longest] = (where[longest] + shift) % entries.shape[longest]
        spots.append(tuple(where))
    return entries.at[spots[0]].set(low).at[spots[1]].set(largest)


def steps_of(key, dims, shards, smallest, high):
    def one(axis_at, parts):
        heights = jax.random.uniform(jax.random.fold_in(jax.random.fold_in(key, 6), axis_at), (parts,), jnp.float32, smallest / len(shards), high / len(shards))
        return jnp.repeat(jnp.exp(heights), dims[axis_at] // parts).reshape((-1,) + (1,) * (len(dims) - axis_at - 1))

    loudness = one(*shards[0])
    for cut in shards[1:]:
        loudness = loudness * one(*cut)
    return loudness


def split_up(count, total, most, lean):
    loads = [(1 << 20) // math.isqrt(grade ** lean) + 1 for grade in range(2, count + 1)]
    surplus, counts = total - most - (count - 1), [1] * (count - 1)
    while surplus > 0:
        movable = [i for i in range(count - 1) if counts[i] < most]
        mass, budget = sum([loads[i] for i in movable]), surplus
        for i in movable:
            addition = min(most - counts[i], max(1, budget * loads[i] // mass), surplus)
            counts[i] = counts[i] + addition
            surplus = surplus - addition
    return np.array([most] + counts)


def uneven_parts(own_key, number_of, total, most, skew):
    if number_of == 2:
        one = jax.random.randint(own_key, (), max(1, total - most), min(most, total - 1) + 1)
        return jnp.stack([one, total - one])
    tallies = jnp.asarray(split_up(number_of, total, most, skew), jnp.int32)
    pairs = (number_of - 1) // 2
    source_of, taker = tallies[1:1 + 2 * pairs:2], tallies[2:2 + 2 * pairs:2]
    margin = jnp.minimum(source_of - 1, most - taker)
    shifted = jax.random.randint(jax.random.fold_in(own_key, 1), (pairs,), 0, 1 << 20) % (margin + 1)
    tallies = tallies.at[1:1 + 2 * pairs:2].set(source_of - shifted).at[2:2 + 2 * pairs:2].set(taker + shifted)
    return tallies[jax.random.permutation(jax.random.fold_in(own_key, 2), number_of)]


def bell_draw(key, shape, spread, reach, split=(), kind=jnp.bfloat16):
    drawn = spread * jax.random.normal(key, shape, jnp.float32)
    if split:
        drawn = drawn * steps_of(key, shape, split, -0.22, 0.18)
    return jnp.clip(drawn, -reach, reach).astype(kind)


def setup_inputs(seed: int = 0) -> dict:
    arg_keys = jax.random.split(jax.random.key(seed), 10)
    return {
        "queries": bell_draw(arg_keys[0], (SEQ, HEADS * D_HEAD), 1.0, 6.0, ((0, 16), (1, 16))),
        "keys": bell_draw(arg_keys[1], (SEQ, KV_HEADS * D_HEAD), 1.0, 6.0, ((0, 256),)),
        "values": bell_draw(arg_keys[2], (SEQ, KV_HEADS * D_HEAD), 0.5, 3.0, ((0, 256),)),
        "attn_out": bell_draw(arg_keys[3], (SEQ, HEADS * D_HEAD), 0.3, 1.796875, ((0, 16), (1, 16))),
        "out_grad": bell_draw(arg_keys[4], (SEQ, HEADS * D_HEAD), 1.0, 6.0, ((0, 16), (1, 16))),
        "log_norm": jnp.clip(3.5 + 2.0 * jax.random.uniform(arg_keys[5], (HEADS, SEQ), jnp.float32) ** steps_of(arg_keys[5], (HEADS, SEQ), ((0, 16), (1, 16)), -0.2, 0.2), 3.5, 5.5),
        "block_layout": touch_ends((jax.random.randint(arg_keys[6], (HEADS, NBLK, NBLK), 0, 4) < 3).astype(jnp.int32), jax.random.fold_in(arg_keys[6], 1), 0, 1),
        "document_ids": jnp.searchsorted(jnp.cumsum(uneven_parts(arg_keys[7], DOCS, SEQ, SEQ // 2, 2)), jnp.arange(SEQ), side="right").astype(jnp.int32),
        "block_order": jax.random.permutation(arg_keys[8], NBLK).astype(jnp.int32),
    }


def stored_positions(block_order, document_ids):
    stored = jnp.arange(SEQ, dtype=jnp.int32)
    position = block_order[stored // BLOCK].astype(jnp.int32) * BLOCK + stored % BLOCK
    return position, document_ids[position]


def reference(queries, keys, values, attn_out, out_grad, log_norm, block_layout, document_ids, block_order):
    position, docs = stored_positions(block_order, document_ids)
    blocks = position // BLOCK
    scaling = D_HEAD ** -0.5
    allowed = (position[None, :] <= position[:, None]) & (docs[:, None] == docs[None, :])
    query_heads = queries.reshape(SEQ, HEADS, D_HEAD).transpose(1, 0, 2)
    grad_heads = out_grad.reshape(SEQ, HEADS, D_HEAD).transpose(1, 0, 2)
    out_heads = attn_out.reshape(SEQ, HEADS, D_HEAD).transpose(1, 0, 2)
    key_heads = keys.reshape(SEQ, KV_HEADS, D_HEAD).transpose(1, 0, 2)
    value_heads = values.reshape(SEQ, KV_HEADS, D_HEAD).transpose(1, 0, 2)

    def one_head(head_index):
        query_one = query_heads[head_index]
        grad_one = grad_heads[head_index]
        out_one = out_heads[head_index]
        key_one = key_heads[head_index // GROUP]
        value_one = value_heads[head_index // GROUP]
        layout_one = block_layout[head_index][blocks[:, None], blocks[None, :]] == 1
        visible = allowed & layout_one
        scores = jnp.dot(query_one, key_one.T, preferred_element_type=jnp.float32) * scaling
        weights = jnp.where(visible, jnp.exp(scores - log_norm[head_index][:, None]), 0.0)
        weights_low = weights.astype(jnp.bfloat16)
        value_part = jnp.dot(weights_low.T, grad_one, preferred_element_type=jnp.float32)
        grad_scores = jnp.dot(grad_one, value_one.T, preferred_element_type=jnp.float32)
        delta = jnp.sum(grad_one.astype(jnp.float32) * out_one.astype(jnp.float32), axis=1)
        score_grad = (weights * (grad_scores - delta[:, None])).astype(jnp.bfloat16)
        query_part = jnp.dot(score_grad, key_one, preferred_element_type=jnp.float32)
        key_part = jnp.dot(score_grad.T, query_one, preferred_element_type=jnp.float32)
        return query_part, key_part, value_part

    query_all, key_all, value_all = lax.map(one_head, jnp.arange(HEADS, dtype=jnp.int32))
    query_grad = (query_all * scaling).transpose(1, 0, 2).reshape(SEQ, HEADS * D_HEAD)
    key_sum = key_all.reshape(KV_HEADS, GROUP, SEQ, D_HEAD).sum(axis=1) * scaling
    value_sum = value_all.reshape(KV_HEADS, GROUP, SEQ, D_HEAD).sum(axis=1)
    key_grad = key_sum.transpose(1, 0, 2).reshape(SEQ, KV_HEADS * D_HEAD)
    value_grad = value_sum.transpose(1, 0, 2).reshape(SEQ, KV_HEADS * D_HEAD)
    return (query_grad, key_grad, value_grad)
```

```python
import functools
import math

import jax
import jax.numpy as jnp
from jax import lax
from jax.experimental import pallas as pl
from jax.experimental.pallas import tpu as pltpu
from jax.sharding import Mesh, PartitionSpec as P

D = 128
BLOCK = 128
HALF = 64
SCALE = D ** (-0.5)
LOG2E = math.log2(math.e)
NZ = 8
NQ = 8
NK = 32
DOCS = 8

HEAD = ("x", "w", "p")


def kernel(
    bo, sd, code, meta, q0, g0, qg1, qg2, qg3, a0, a1, a2, a3, *rest
):
    kvs = rest[:NZ]
    dq_out, dkv_out = rest[NZ : NZ + 2]
    qs, gs, rows, kv, acc, pt, dst, kvt, dqt, bks, lhb, lbk, lcd = rest[NZ + 2 :]
    z, c, p = meta[0], meta[1], meta[2]

    for dc in range(2):
        for dp in range(2):
            aux = ((a0, a2), (a1, a3))[dc][dp]
            for b in range(4):
                i = dc * 4 + b
                r = slice(b * BLOCK, (b + 1) * BLOCK)
                for j in range(2):
                    h = dp * 2 + j
                    cols = slice(j * D, (j + 1) * D)
                    gcols = slice(256 + j * D, 256 + (j + 1) * D)
                    hr = slice(h * BLOCK, (h + 1) * BLOCK)
                    if dc == 0 and dp == 0:
                        qs[i, hr, :] = q0[r, cols]
                        gs[i, hr, :] = g0[r, cols]
                    else:
                        src = {(1, 0): qg1, (0, 1): qg2, (1, 1): qg3}[(dc, dp)]
                        qs[i, hr, :] = src[r, cols]
                        gs[i, hr, :] = src[r, gcols]
                    rows[i, 0:1, hr] = aux[j : j + 1, r] * LOG2E
                    rows[i, 1:2, hr] = aux[2 + j : 3 + j, r]
    for k in range(NZ):
        for b in range(4):
            kv[k * 4 + b] = kvs[k][b * HALF : (b + 1) * HALF, :]
        zk = lax.rem(z - k + NZ, NZ)
        for b in range(4):
            bks[k * 4 + b] = bo[4 * (2 * zk + c) + b]
    acc[...] = jnp.zeros_like(acc)

    sub = lax.broadcasted_iota(jnp.int32, (HALF, BLOCK), 0)
    offs = (sub // 16) * 32 + 16 * p + sub % 16
    lane = lax.broadcasted_iota(jnp.int32, (1, BLOCK), 1)

    def query_block(i, _):
        dc = i // 4
        b = lax.rem(i, 4)
        bq = bo[4 * (2 * z + jnp.where(dc == 0, c, 1 - c)) + b]
        first = bq * BLOCK
        start0 = jnp.int32(0)
        pos_row = lane + first
        start_row = jnp.zeros_like(pos_row)
        for d in range(DOCS):
            s = sd[d]
            start0 = jnp.where(s <= first, jnp.maximum(start0, s), start0)
            start_row = jnp.where(s <= pos_row, jnp.maximum(start_row, s), start_row)

        def scan(hb, n):
            bk = bks[hb]
            cd = code[bq, bk]
            act = (bk <= bq) & (bk * BLOCK + BLOCK - 1 >= start0) & (cd != 0)
            lhb[n] = hb
            lbk[n] = bk
            lcd[n] = cd
            return n + act.astype(jnp.int32)

        n = lax.fori_loop(0, NK, scan, jnp.int32(0))
        for e in range(4):
            lhb[n + e] = 0
            lbk[n + e] = 0
            lcd[n + e] = 0
        dqt[...] = jnp.zeros_like(dqt)

        def tile(t, _):
            for m in range(4):
                kvt[m * HALF : (m + 1) * HALF, :] = kv[lhb[4 * t + m]]
            keys = kvt[:, 0:D]
            vals = kvt[:, D : 2 * D]
            nt = (((1,), (1,)), ((), ()))
            st = lax.dot_general(keys, qs[i], nt, preferred_element_type=jnp.float32)
            dpt = lax.dot_general(vals, gs[i], nt, preferred_element_type=jnp.float32)
            for h in range(4):
                hc = slice(h * BLOCK, (h + 1) * BLOCK)
                lse = rows[i, 0:1, hc]
                delta = rows[i, 1:2, hc]
                for m in range(4):
                    mr = slice(m * HALF, (m + 1) * HALF)
                    base = lbk[4 * t + m] * BLOCK
                    bit = (lcd[4 * t + m] >> h) & 1
                    up = jnp.where(bit == 1, pos_row - base, -1)
                    lo = start_row - base
                    mask = (offs <= up) & (offs >= lo)
                    w = jnp.where(mask, jnp.exp2(st[mr, hc] * (SCALE * LOG2E) - lse), 0.0)
                    pt[mr, hc] = w.astype(jnp.bfloat16)
                    dst[mr, hc] = (w * (dpt[mr, hc] - delta)).astype(jnp.bfloat16)
            nn = (((1,), (0,)), ((), ()))
            dk = lax.dot_general(dst[...], qs[i], nn, preferred_element_type=jnp.float32)
            dv = lax.dot_general(pt[...], gs[i], nn, preferred_element_type=jnp.float32)
            dqt[...] += lax.dot_general(
                keys, dst[...], (((0,), (0,)), ((), ())), preferred_element_type=jnp.float32
            )
            for m in range(4):
                mr = slice(m * HALF, (m + 1) * HALF)
                hb = lhb[4 * t + m]
                acc[hb, :, 0:D] += dk[mr, :]
                acc[hb, :, D : 2 * D] += dv[mr, :]
            return 0

        lax.fori_loop(0, (n + 3) // 4, tile, 0)
        dq = dqt[...].T * SCALE
        for dp in range(2):
            for j in range(2):
                h = dp * 2 + j
                dq_out[dc, dp, b, :, j * D : (j + 1) * D] = dq[h * BLOCK : (h + 1) * BLOCK, :]
        return 0

    lax.fori_loop(0, NQ, query_block, 0)
    for k in range(NZ):
        zk = lax.rem(z - k + NZ, NZ)
        for b in range(4):
            br = slice(b * HALF, (b + 1) * HALF)
            dkv_out[zk, br, 0:D] = (acc[k * 4 + b, :, 0:D] * SCALE).astype(jnp.bfloat16)
            dkv_out[zk, br, D : 2 * D] = acc[k * 4 + b, :, D : 2 * D].astype(jnp.bfloat16)


def attend(bo, sd, code, meta, qg, aux, kvs):
    smem = pl.BlockSpec(memory_space=pltpu.SMEM)
    vmem = pl.BlockSpec(memory_space=pltpu.VMEM)
    rows = 4 * BLOCK
    return pl.pallas_call(
        kernel,
        in_specs=[smem] * 4 + [vmem] * (5 + 4 + NZ),
        out_specs=[vmem, vmem],
        out_shape=[
            jax.ShapeDtypeStruct((2, 2, 4, BLOCK, 2 * D), jnp.float32),
            jax.ShapeDtypeStruct((NZ, 4 * HALF, 2 * D), jnp.bfloat16),
        ],
        scratch_shapes=[
            pltpu.VMEM((NQ, rows, D), jnp.bfloat16),
            pltpu.VMEM((NQ, rows, D), jnp.bfloat16),
            pltpu.VMEM((NQ, 8, rows), jnp.float32),
            pltpu.VMEM((NK, HALF, 2 * D), jnp.bfloat16),
            pltpu.VMEM((NK, HALF, 2 * D), jnp.float32),
            pltpu.VMEM((4 * HALF, rows), jnp.bfloat16),
            pltpu.VMEM((4 * HALF, rows), jnp.bfloat16),
            pltpu.VMEM((4 * HALF, 2 * D), jnp.bfloat16),
            pltpu.VMEM((D, rows), jnp.float32),
            pltpu.SMEM((NK,), jnp.int32),
            pltpu.SMEM((NK + 8,), jnp.int32),
            pltpu.SMEM((NK + 8,), jnp.int32),
            pltpu.SMEM((NK + 8,), jnp.int32),
        ],
        compiler_params=pltpu.CompilerParams(vmem_limit_bytes=40 * 1024 * 1024),
        name="attend",
    )(bo, sd, code, meta, *qg, *aux, *kvs)


SWAP = [(0, 1), (1, 0)]


def turn(k):
    return [(i, (i + k) % NZ) for i in range(NZ)]


def body(
    queries, keys, values, attn_out, out_grad, log_norm, block_layout, document_ids, block_order
):
    z = lax.axis_index("z")
    c = lax.axis_index("c")
    p = lax.axis_index("p")
    meta = jnp.stack([z, c, p]).astype(jnp.int32)

    k = keys.reshape(2, 16, 8, D).transpose(2, 0, 1, 3)
    v = values.reshape(2, 16, 8, D).transpose(2, 0, 1, 3)
    kv = jnp.concatenate([k, v], axis=3).reshape(16, 16, 2 * D)
    qg0 = jnp.concatenate([queries, out_grad], axis=1)
    qg2 = lax.ppermute(qg0, "p", SWAP)
    kv = lax.all_to_all(kv, HEAD, 0, 0, tiled=True).reshape(256, 2 * D)
    kvs = [kv] + [None] * 7
    for kk in (4, 3, 5, 2, 6, 1, 7):
        kvs[kk] = lax.ppermute(kv, "z", turn(kk))

    delta = jnp.sum(
        (out_grad.astype(jnp.float32) * attn_out.astype(jnp.float32)).reshape(512, 2, D), axis=2
    ).T
    aux0 = jnp.concatenate([log_norm, delta], axis=0)
    aux2 = lax.ppermute(aux0, "p", SWAP)
    code0 = block_layout[0] + 2 * block_layout[1]
    code2 = lax.ppermute(code0, "p", SWAP)
    code = code0 + 4 * code2
    qg1 = lax.ppermute(qg0, "c", SWAP)
    qg3 = lax.ppermute(qg2, "c", SWAP)
    aux1 = lax.ppermute(aux0, "c", SWAP)
    aux3 = lax.ppermute(aux2, "c", SWAP)
    docs = jnp.arange(DOCS, dtype=jnp.int32)
    sd = jnp.sum((document_ids[None, :] < docs[:, None]).astype(jnp.int32), axis=1)

    dq, dkv = attend(
        block_order, sd, code, meta,
        (queries, out_grad, qg1, qg2, qg3), (aux0, aux1, aux2, aux3), kvs,
    )
    other = lax.ppermute(dq[1], "c", SWAP)
    dq = dq[0] + other
    far = lax.ppermute(dq[1], "p", SWAP)
    query_grad = (dq[0] + far).reshape(512, 2 * D)

    parts = lax.all_to_all(dkv, "z", 0, 0, tiled=True)
    total = jnp.sum(parts.astype(jnp.float32), axis=0)
    out = lax.all_to_all(total.reshape(16, 16, 2 * D), HEAD, 0, 0, tiled=True)
    out = out.reshape(8, 2, 16, 2 * D).transpose(1, 2, 0, 3)
    key_grad = out[..., :D].reshape(32, 8 * D)
    value_grad = out[..., D:].reshape(32, 8 * D)
    return query_grad, key_grad, value_grad


def solution(mesh):
    fine = Mesh(mesh.devices.reshape(NZ, 2, 4, 2, 2), ("z", "c") + HEAD)
    seq = ("z", "c")
    in_specs = (
        P(seq, HEAD),
        P(seq + HEAD, None),
        P(seq + HEAD, None),
        P(seq, HEAD),
        P(seq, HEAD),
        P(HEAD, seq),
        P(HEAD, None, None),
        P(),
        P(),
    )
    out_specs = (P(seq, HEAD), P(seq + HEAD, None), P(seq + HEAD, None))
    return jax.shard_map(body, mesh=fine, in_specs=in_specs, out_specs=out_specs, check_vma=False)
```

```python
import math

import jax
import jax.numpy as jnp
from jax import lax
from jax.experimental import pallas as pl
from jax.experimental.pallas import tpu as pltpu
from jax.sharding import Mesh, PartitionSpec as P

D = 128
BLOCK = 128
HALF = 64
CHUNK = 4 * HALF
SCALE = D ** (-0.5)
LOG2E = math.log2(math.e)
NZ = 8
NQ = 8
ROWS = 4 * BLOCK
DOCS = 8
UNROLL = 3
FIRST = (0, 4, 3, 5)
SECOND = (2, 6, 1, 7)
INS = FIRST[1:] + SECOND

HEAD = ("x", "w", "p")


def make_kernel(offsets, first):
    nc = len(offsets)
    nk = 4 * nc

    def kernel(bo, sd, code, meta, *refs):
        if first:
            q0, g0, qg1, qg2, qg3 = refs[:5]
            refs = refs[5:]
        else:
            qs, gs, dq_in = refs[:3]
            refs = refs[3:]
        a0, a1, a2, a3 = refs[:4]
        refs = refs[4:]
        kvs, refs = refs[:nc], refs[nc:]
        dqt, refs = refs[0], refs[1:]
        outs, refs = refs[:nc], refs[nc:]
        if first:
            qs, gs, refs = refs[0], refs[1], refs[2:]
        rows, spans, kv, acc, pt, dst, kvt, tags, lst, sem = refs
        z, c, p = meta[0], meta[1], meta[2]

        copies = []
        for dc in range(2):
            for dp in range(2):
                aux = ((a0, a2), (a1, a3))[dc][dp]
                for b in range(4):
                    i = dc * 4 + b
                    r = pl.ds(b * BLOCK, BLOCK)
                    for j in range(2):
                        h = dp * 2 + j
                        hr = pl.ds(h * BLOCK, BLOCK)
                        srcs = ()
                        if first and dc == 0 and dp == 0:
                            srcs = ((q0, 0, qs), (g0, 0, gs))
                        elif first:
                            sq = {(1, 0): qg1, (0, 1): qg2, (1, 1): qg3}[(dc, dp)]
                            srcs = ((sq, 0, qs), (sq, 2 * D, gs))
                        for src, o, dest in srcs:
                            cp = pltpu.make_async_copy(
                                src.at[r, pl.ds(o + j * D, D)], dest.at[i, hr, :], sem
                            )
                            cp.start()
                            copies.append(cp)
                        rs = slice(b * BLOCK, (b + 1) * BLOCK)
                        hs = slice(h * BLOCK, (h + 1) * BLOCK)
                        rows[i, 0:1, hs] = aux[j : j + 1, rs] * LOG2E
                        rows[i, 1:2, hs] = aux[2 + j : 3 + j, rs]
        for n, k in enumerate(offsets):
            cp = pltpu.make_async_copy(kvs[n], kv.at[pl.ds(n * CHUNK, CHUNK), :], sem)
            cp.start()
            copies.append(cp)
            zk = lax.rem(z - k + NZ, NZ)
            for b in range(4):
                hb = n * 4 + b
                tags[hb] = hb + (bo[4 * (2 * zk + c) + b] << 8)
        acc[...] = jnp.zeros_like(acc)
        if first:
            dqt[...] = jnp.zeros_like(dqt)
        else:
            dqt[...] = dq_in[...]

        sub = lax.broadcasted_iota(jnp.int32, (HALF, BLOCK), 0)
        offs = (sub // 16) * 32 + 16 * p + sub % 16
        lane = lax.broadcasted_iota(jnp.int32, (1, BLOCK), 1)

        def scan(i, n):
            cq = jnp.where(i < 4, c, 1 - c)
            bq = bo[4 * (2 * z + cq) + (i & 3)]
            head = bq * BLOCK
            start0 = jnp.int32(0)
            pos_row = lane + head
            start_row = jnp.zeros_like(pos_row)
            for d in range(DOCS):
                s = sd[d]
                start0 = jnp.where(s <= head, jnp.maximum(start0, s), start0)
                start_row = jnp.where(s <= pos_row, jnp.maximum(start_row, s), start_row)
            spans[i, 0:1, :] = pos_row
            spans[i, 1:2, :] = start_row
            b0 = start0 // BLOCK
            mark = i << 20
            for hb in range(nk):
                tag = tags[hb]
                bk = tag >> 8
                cd = code[bq, bk]
                act = (bk <= bq) & (bk >= b0) & (cd != 0)
                lst[n] = tag + (cd << 16) + mark
                n = n + act.astype(jnp.int32)
            for e in range(3):
                lst[n + e] = mark
            return (n + 3) & -4

        n = lax.fori_loop(0, NQ, scan, jnp.int32(0))
        for e in range(4 * (UNROLL - 1)):
            lst[n + e] = 0
        for cp in copies:
            cp.wait()

        def tile(t, u):
            hbs, bases, bits = [], [], []
            i = lst[4 * t] >> 20
            for m in range(4):
                word = lst[4 * t + m]
                hb = pl.multiple_of((word & 255) * HALF, HALF)
                hbs.append(hb)
                bases.append(((word >> 8) & 255) * BLOCK)
                bits.append(word >> 16)
                kvt[u, m * HALF : (m + 1) * HALF, :] = kv[pl.ds(hb, HALF), :]
            keys = kvt[u, :, 0:D]
            vals = kvt[u, :, D : 2 * D]
            pos_row = spans[i, 0:1, :]
            start_row = spans[i, 1:2, :]
            nt = (((1,), (1,)), ((), ()))
            st = lax.dot_general(keys, qs[i], nt, preferred_element_type=jnp.float32)
            dpt = lax.dot_general(vals, gs[i], nt, preferred_element_type=jnp.float32)
            for h in range(4):
                hc = slice(h * BLOCK, (h + 1) * BLOCK)
                lse = rows[i, 0:1, hc]
                delta = rows[i, 1:2, hc]
                for m in range(4):
                    mr = slice(m * HALF, (m + 1) * HALF)
                    up = jnp.where((bits[m] >> h) & 1 == 1, pos_row - bases[m], -1)
                    lo = start_row - bases[m]
                    mask = (offs <= up) & (offs >= lo)
                    w = jnp.where(mask, jnp.exp2(st[mr, hc] * (SCALE * LOG2E) - lse), 0.0)
                    pt[u, mr, hc] = w.astype(jnp.bfloat16)
                    dst[u, mr, hc] = (w * (dpt[mr, hc] - delta)).astype(jnp.bfloat16)
            nn = (((1,), (0,)), ((), ()))
            dk = lax.dot_general(dst[u], qs[i], nn, preferred_element_type=jnp.float32)
            dv = lax.dot_general(pt[u], gs[i], nn, preferred_element_type=jnp.float32)
            dq = lax.dot_general(
                keys, dst[u], (((0,), (0,)), ((), ())), preferred_element_type=jnp.float32
            )
            return i, hbs, dk, dv, dq

        def tiles(t, _):
            done = [tile(UNROLL * t + u, u) for u in range(UNROLL)]
            for i, hbs, dk, dv, dq in done:
                dqt[i] += dq
                for m in range(4):
                    mr = slice(m * HALF, (m + 1) * HALF)
                    acc[pl.ds(hbs[m], HALF), 0:D] += dk[mr, :]
                    acc[pl.ds(hbs[m], HALF), D : 2 * D] += dv[mr, :]
            return 0

        lax.fori_loop(0, (n // 4 + UNROLL - 1) // UNROLL, tiles, 0)

        for n in range(nc):
            cr = slice(n * CHUNK, (n + 1) * CHUNK)
            dest = outs[n]
            dest[:, 0:D] = (acc[cr, 0:D] * SCALE).astype(dest.dtype)
            dest[:, D : 2 * D] = acc[cr, D : 2 * D].astype(dest.dtype)

    return kernel


def attend(offsets, first, bo, sd, code, meta, aux, kvs, before):
    nc = len(offsets)
    smem = pl.BlockSpec(memory_space=pltpu.SMEM)
    vmem = pl.BlockSpec(memory_space=pltpu.VMEM)
    hbm = pl.BlockSpec(memory_space=pltpu.HBM)
    shapes = [jax.ShapeDtypeStruct((NQ, D, ROWS), jnp.float32)] + [
        jax.ShapeDtypeStruct((CHUNK, 2 * D), jnp.bfloat16 if k else jnp.float32) for k in offsets
    ]
    if first:
        shapes += [jax.ShapeDtypeStruct((NQ, ROWS, D), jnp.bfloat16)] * 2
    return pl.pallas_call(
        make_kernel(offsets, first),
        in_specs=[smem] * 4 + [hbm if first else vmem] * len(before) + [vmem] * 4 + [hbm] * nc,
        out_specs=[vmem] * len(shapes),
        out_shape=shapes,
        scratch_shapes=[
            pltpu.VMEM((NQ, 8, ROWS), jnp.float32),
            pltpu.VMEM((NQ, 8, BLOCK), jnp.int32),
            pltpu.VMEM((nc * CHUNK, 2 * D), jnp.bfloat16),
            pltpu.VMEM((nc * CHUNK, 2 * D), jnp.float32),
            pltpu.VMEM((UNROLL, CHUNK, ROWS), jnp.bfloat16),
            pltpu.VMEM((UNROLL, CHUNK, ROWS), jnp.bfloat16),
            pltpu.VMEM((UNROLL, CHUNK, 2 * D), jnp.bfloat16),
            pltpu.SMEM((4 * nc,), jnp.int32),
            pltpu.SMEM((NQ * 4 * nc + 4 * UNROLL + 4,), jnp.int32),
            pltpu.SemaphoreType.DMA,
        ],
        compiler_params=pltpu.CompilerParams(vmem_limit_bytes=16 * 1024 * 1024),
        name="attend_first" if first else "attend_second",
    )(bo, sd, code, meta, *before, *aux, *kvs)


def pack_kernel(keys_in, values_in, out, keys, values, sem):
    copies = [pltpu.make_async_copy(keys_in, keys, sem), pltpu.make_async_copy(values_in, values, sem)]
    for cp in copies:
        cp.start()
    for cp in copies:
        cp.wait()
    for g in range(8):
        for half in range(2):
            r, cols = slice(16 * half, 16 * half + 16), slice(g * D, (g + 1) * D)
            out[2 * g + half, :, 0:D] = keys[r, cols]
            out[2 * g + half, :, D : 2 * D] = values[r, cols]


def flip_kernel(dq, other, mate, out):
    for b in range(4):
        for j in range(2):
            cols = slice(j * BLOCK, (j + 1) * BLOCK)
            part = dq[b, :, cols] + other[b, :, cols] + mate[b, :, cols].astype(jnp.float32)
            out[b * BLOCK : (b + 1) * BLOCK, j * D : (j + 1) * D] = part.T * SCALE


def flip(dq, other, mate):
    half = pl.BlockSpec((4, D, 2 * BLOCK), lambda i: (0, 0, 0))
    return pl.pallas_call(
        flip_kernel,
        grid=(1,),
        in_specs=[half] * 3,
        out_specs=pl.BlockSpec((4 * BLOCK, 2 * D), lambda i: (0, 0)),
        out_shape=jax.ShapeDtypeStruct((4 * BLOCK, 2 * D), jnp.float32),
        compiler_params=pltpu.CompilerParams(vmem_limit_bytes=8 * 1024 * 1024),
        name="flip",
    )(dq, other, mate)


def pack(keys, values):
    hbm = pl.BlockSpec(memory_space=pltpu.HBM)
    return pl.pallas_call(
        pack_kernel,
        in_specs=[hbm, hbm],
        out_specs=pl.BlockSpec(memory_space=pltpu.VMEM),
        scratch_shapes=[
            pltpu.VMEM(keys.shape, keys.dtype),
            pltpu.VMEM(values.shape, values.dtype),
            pltpu.SemaphoreType.DMA,
        ],
        out_shape=jax.ShapeDtypeStruct((16, 16, 2 * D), jnp.bfloat16),
        compiler_params=pltpu.CompilerParams(vmem_limit_bytes=4 * 1024 * 1024),
        name="pack",
    )(keys, values)


SWAP = [(0, 1), (1, 0)]


def turn(k):
    return [(i, (i + k) % NZ) for i in range(NZ)]


def body(
    queries, keys, values, attn_out, out_grad, log_norm, block_layout, document_ids, block_order
):
    z = lax.axis_index("z")
    c = lax.axis_index("c")
    p = lax.axis_index("p")
    meta = jnp.stack([z, c, p]).astype(jnp.int32)

    kv = pack(keys, values)
    kv = lax.all_to_all(kv, HEAD, 0, 0, tiled=True).reshape(CHUNK, 2 * D)
    kvs = {0: kv}
    for kk in INS:
        kvs[kk] = lax.ppermute(kv, "z", turn(kk))

    qg0 = jnp.concatenate([queries, out_grad], axis=1)
    qg2 = lax.ppermute(qg0, "p", SWAP)
    qg1 = lax.ppermute(qg0, "c", SWAP)
    qg3 = lax.ppermute(qg2, "c", SWAP)
    delta = jnp.sum(
        (out_grad.astype(jnp.float32) * attn_out.astype(jnp.float32)).reshape(512, 2, D), axis=2
    ).T
    aux0 = jnp.concatenate([log_norm, delta], axis=0)
    aux2 = lax.ppermute(aux0, "p", SWAP)
    aux1 = lax.ppermute(aux0, "c", SWAP)
    aux3 = lax.ppermute(aux2, "c", SWAP)
    code0 = block_layout[0] + 2 * block_layout[1]
    code2 = lax.ppermute(code0, "p", SWAP)
    code = code0 + 4 * code2
    docs = jnp.arange(DOCS, dtype=jnp.int32)
    sd = jnp.sum((document_ids[None, :] < docs[:, None]).astype(jnp.int32), axis=1)

    common = (block_order, sd, code, meta, (aux0, aux1, aux2, aux3))
    pooled = (queries, out_grad, qg1, qg2, qg3)
    dq, own, *parts, qs, gs = attend(FIRST, True, *common, [kvs[kk] for kk in FIRST], pooled)
    back = {}
    for kk, part in zip(FIRST[1:], parts):
        back[kk] = lax.ppermute(part, "z", turn(-kk))
    dq, *parts = attend(SECOND, False, *common, [kvs[kk] for kk in SECOND], (qs, gs, dq))
    other = lax.ppermute(dq[4:], "c", SWAP)
    high = (dq[:4, :, 2 * BLOCK :] + other[:, :, 2 * BLOCK :]).astype(jnp.bfloat16)
    parts[-1], high = lax.optimization_barrier((parts[-1], high))
    for kk, part in zip(SECOND, parts):
        back[kk] = lax.ppermute(part, "z", turn(-kk))
    mate = lax.ppermute(high, "p", SWAP)
    query_grad = flip(dq, other, mate)

    total = own
    for kk in INS:
        total = total + back[kk].astype(jnp.float32)
    out = lax.all_to_all(total.reshape(16, 16, 2 * D), HEAD, 0, 0, tiled=True)
    out = out.reshape(8, 2, 16, 2 * D).transpose(1, 2, 0, 3)
    key_grad = out[..., :D].reshape(32, 8 * D)
    value_grad = out[..., D:].reshape(32, 8 * D)
    return query_grad, key_grad, value_grad


def solution(mesh):
    fine = Mesh(mesh.devices.reshape(NZ, 2, 4, 2, 2), ("z", "c") + HEAD)
    seq = ("z", "c")
    in_specs = (
        P(seq, HEAD),
        P(seq + HEAD, None),
        P(seq + HEAD, None),
        P(seq, HEAD),
        P(seq, HEAD),
        P(HEAD, seq),
        P(HEAD, None, None),
        P(),
        P(),
    )
    out_specs = (P(seq, HEAD), P(seq + HEAD, None), P(seq + HEAD, None))

    return jax.shard_map(body, mesh=fine, in_specs=in_specs, out_specs=out_specs, check_vma=False)
```

```python
import math

import jax
import jax.numpy as jnp
from jax import lax
from jax.experimental import pallas as pl
from jax.experimental.pallas import tpu as pltpu
from jax.sharding import Mesh, PartitionSpec as P

D = 128
BLOCK = 128
HALF = 64
CHUNK = 4 * HALF
SCALE = D ** (-0.5)
LOG2E = math.log2(math.e)
NZ = 8
NQ = 8
ROWS = 4 * BLOCK
DOCS = 8
UNROLL = 3
FIRST = (0, 4, 3, 5)
SECOND = (2, 6, 1, 7)
INS = FIRST[1:] + SECOND

HEAD = ("x", "w", "p")


def make_kernel(offsets, first):
    nc = len(offsets)
    nk = 4 * nc

    def kernel(bo, sd, code, meta, *refs):
        if first:
            q0, g0, qg1, qg2, qg3 = refs[:5]
            refs = refs[5:]
        else:
            qs, gs, dq_in = refs[:3]
            refs = refs[3:]
        a0, a1, a2, a3 = refs[:4]
        refs = refs[4:]
        kvs, refs = refs[:nc], refs[nc:]
        dqt, refs = refs[0], refs[1:]
        outs, refs = refs[:nc], refs[nc:]
        if first:
            qs, gs, refs = refs[0], refs[1], refs[2:]
        rows, spans, kv, acc, pt, dst, kvt, tags, lst, sem = refs
        z, c, p = meta[0], meta[1], meta[2]

        copies = []
        for dc in range(2):
            for dp in range(2):
                aux = ((a0, a2), (a1, a3))[dc][dp]
                for b in range(4):
                    i = dc * 4 + b
                    r = pl.ds(b * BLOCK, BLOCK)
                    for j in range(2):
                        h = dp * 2 + j
                        hr = pl.ds(h * BLOCK, BLOCK)
                        srcs = ()
                        if first and dc == 0 and dp == 0:
                            srcs = ((q0, 0, qs), (g0, 0, gs))
                        elif first:
                            sq = {(1, 0): qg1, (0, 1): qg2, (1, 1): qg3}[(dc, dp)]
                            srcs = ((sq, 0, qs), (sq, 2 * D, gs))
                        for src, o, dest in srcs:
                            cp = pltpu.make_async_copy(
                                src.at[r, pl.ds(o + j * D, D)], dest.at[i, hr, :], sem
                            )
                            cp.start()
                            copies.append(cp)
                        rs = slice(b * BLOCK, (b + 1) * BLOCK)
                        hs = slice(h * BLOCK, (h + 1) * BLOCK)
                        rows[i, 0:1, hs] = aux[j : j + 1, rs] * LOG2E
                        rows[i, 1:2, hs] = aux[2 + j : 3 + j, rs]
        for n, k in enumerate(offsets):
            kv[n * CHUNK : (n + 1) * CHUNK, :] = kvs[n][...]
            zk = lax.rem(z - k + NZ, NZ)
            for b in range(4):
                hb = n * 4 + b
                tags[hb] = hb + (bo[4 * (2 * zk + c) + b] << 8)
        acc[...] = jnp.zeros_like(acc)
        if first:
            dqt[...] = jnp.zeros_like(dqt)
        else:
            dqt[...] = dq_in[...]

        sub = lax.broadcasted_iota(jnp.int32, (HALF, BLOCK), 0)
        offs = (sub // 16) * 32 + 16 * p + sub % 16
        lane = lax.broadcasted_iota(jnp.int32, (1, BLOCK), 1)

        def scan(i, n):
            cq = jnp.where(i < 4, c, 1 - c)
            bq = bo[4 * (2 * z + cq) + (i & 3)]
            head = bq * BLOCK
            start0 = jnp.int32(0)
            pos_row = lane + head
            start_row = jnp.zeros_like(pos_row)
            for d in range(DOCS):
                s = sd[d]
                start0 = jnp.where(s <= head, jnp.maximum(start0, s), start0)
                start_row = jnp.where(s <= pos_row, jnp.maximum(start_row, s), start_row)
            spans[i, 0:1, :] = pos_row
            spans[i, 1:2, :] = start_row
            b0 = start0 // BLOCK
            mark = i << 20
            for hb in range(nk):
                tag = tags[hb]
                bk = tag >> 8
                cd = code[bq, bk]
                act = (bk <= bq) & (bk >= b0) & (cd != 0)
                lst[n] = tag + (cd << 16) + mark
                n = n + act.astype(jnp.int32)
            for e in range(3):
                lst[n + e] = mark
            return (n + 3) & -4

        n = lax.fori_loop(0, NQ, scan, jnp.int32(0))
        for e in range(4 * (UNROLL - 1)):
            lst[n + e] = 0
        for cp in copies:
            cp.wait()

        def tile(t, u):
            hbs, bases, bits = [], [], []
            i = lst[4 * t] >> 20
            for m in range(4):
                word = lst[4 * t + m]
                hb = pl.multiple_of((word & 255) * HALF, HALF)
                hbs.append(hb)
                bases.append(((word >> 8) & 255) * BLOCK)
                bits.append(word >> 16)
                kvt[u, m * HALF : (m + 1) * HALF, :] = kv[pl.ds(hb, HALF), :]
            keys = kvt[u, :, 0:D]
            vals = kvt[u, :, D : 2 * D]
            pos_row = spans[i, 0:1, :]
            start_row = spans[i, 1:2, :]
            nt = (((1,), (1,)), ((), ()))
            st = lax.dot_general(keys, qs[i], nt, preferred_element_type=jnp.float32)
            dpt = lax.dot_general(vals, gs[i], nt, preferred_element_type=jnp.float32)
            for h in range(4):
                hc = slice(h * BLOCK, (h + 1) * BLOCK)
                lse = rows[i, 0:1, hc]
                delta = rows[i, 1:2, hc]
                for m in range(4):
                    mr = slice(m * HALF, (m + 1) * HALF)
                    up = jnp.where((bits[m] >> h) & 1 == 1, pos_row - bases[m], -1)
                    lo = start_row - bases[m]
                    mask = (offs <= up) & (offs >= lo)
                    w = jnp.where(mask, jnp.exp2(st[mr, hc] * (SCALE * LOG2E) - lse), 0.0)
                    pt[u, mr, hc] = w.astype(jnp.bfloat16)
                    dst[u, mr, hc] = (w * (dpt[mr, hc] - delta)).astype(jnp.bfloat16)
            nn = (((1,), (0,)), ((), ()))
            dk = lax.dot_general(dst[u], qs[i], nn, preferred_element_type=jnp.float32)
            dv = lax.dot_general(pt[u], gs[i], nn, preferred_element_type=jnp.float32)
            dq = lax.dot_general(
                keys, dst[u], (((0,), (0,)), ((), ())), preferred_element_type=jnp.float32
            )
            return i, hbs, dk, dv, dq

        def tiles(t, _):
            done = [tile(UNROLL * t + u, u) for u in range(UNROLL)]
            for i, hbs, dk, dv, dq in done:
                dqt[i] += dq
                for m in range(4):
                    mr = slice(m * HALF, (m + 1) * HALF)
                    acc[pl.ds(hbs[m], HALF), 0:D] += dk[mr, :]
                    acc[pl.ds(hbs[m], HALF), D : 2 * D] += dv[mr, :]
            return 0

        lax.fori_loop(0, (n // 4 + UNROLL - 1) // UNROLL, tiles, 0)

        for n in range(nc):
            cr = slice(n * CHUNK, (n + 1) * CHUNK)
            dest = outs[n]
            dest[:, 0:D] = (acc[cr, 0:D] * SCALE).astype(dest.dtype)
            dest[:, D : 2 * D] = acc[cr, D : 2 * D].astype(dest.dtype)

    return kernel


def attend(offsets, first, bo, sd, code, meta, aux, kvs, before):
    nc = len(offsets)
    smem = pl.BlockSpec(memory_space=pltpu.SMEM)
    vmem = pl.BlockSpec(memory_space=pltpu.VMEM)
    hbm = pl.BlockSpec(memory_space=pltpu.HBM)
    shapes = [jax.ShapeDtypeStruct((NQ, D, ROWS), jnp.float32)] + [
        jax.ShapeDtypeStruct((CHUNK, 2 * D), jnp.bfloat16 if k else jnp.float32) for k in offsets
    ]
    if first:
        shapes += [jax.ShapeDtypeStruct((NQ, ROWS, D), jnp.bfloat16)] * 2
    return pl.pallas_call(
        make_kernel(offsets, first),
        in_specs=[smem] * 4 + [hbm if first else vmem] * len(before) + [vmem] * (4 + nc),
        out_specs=[vmem] * len(shapes),
        out_shape=shapes,
        scratch_shapes=[
            pltpu.VMEM((NQ, 8, ROWS), jnp.float32),
            pltpu.VMEM((NQ, 8, BLOCK), jnp.int32),
            pltpu.VMEM((nc * CHUNK, 2 * D), jnp.bfloat16),
            pltpu.VMEM((nc * CHUNK, 2 * D), jnp.float32),
            pltpu.VMEM((UNROLL, CHUNK, ROWS), jnp.bfloat16),
            pltpu.VMEM((UNROLL, CHUNK, ROWS), jnp.bfloat16),
            pltpu.VMEM((UNROLL, CHUNK, 2 * D), jnp.bfloat16),
            pltpu.SMEM((4 * nc,), jnp.int32),
            pltpu.SMEM((NQ * 4 * nc + 4 * UNROLL + 4,), jnp.int32),
            pltpu.SemaphoreType.DMA,
        ],
        compiler_params=pltpu.CompilerParams(vmem_limit_bytes=16 * 1024 * 1024),
        name="attend_first" if first else "attend_second",
    )(bo, sd, code, meta, *before, *aux, *kvs)


def pack_kernel(keys_in, values_in, out, keys, values, sem):
    copies = [pltpu.make_async_copy(keys_in, keys, sem), pltpu.make_async_copy(values_in, values, sem)]
    for cp in copies:
        cp.start()
    for cp in copies:
        cp.wait()
    for g in range(8):
        for half in range(2):
            r, cols = slice(16 * half, 16 * half + 16), slice(g * D, (g + 1) * D)
            out[2 * g + half, :, 0:D] = keys[r, cols]
            out[2 * g + half, :, D : 2 * D] = values[r, cols]


def flip_kernel(dq, other, mate, out):
    for b in range(4):
        for j in range(2):
            cols = slice(j * BLOCK, (j + 1) * BLOCK)
            part = dq[b, :, cols] + other[b, :, cols] + mate[b, :, cols].astype(jnp.float32)
            out[b * BLOCK : (b + 1) * BLOCK, j * D : (j + 1) * D] = part.T * SCALE


def flip(dq, other, mate):
    half = pl.BlockSpec((4, D, 2 * BLOCK), lambda i: (0, 0, 0))
    return pl.pallas_call(
        flip_kernel,
        grid=(1,),
        in_specs=[half] * 3,
        out_specs=pl.BlockSpec((4 * BLOCK, 2 * D), lambda i: (0, 0)),
        out_shape=jax.ShapeDtypeStruct((4 * BLOCK, 2 * D), jnp.float32),
        compiler_params=pltpu.CompilerParams(vmem_limit_bytes=8 * 1024 * 1024),
        name="flip",
    )(dq, other, mate)


def unpack_kernel(parts, keys, values):
    for g in range(8):
        for half in range(2):
            r, cols = slice(16 * half, 16 * half + 16), slice(g * D, (g + 1) * D)
            keys[r, cols] = parts[2 * g + half, :, 0:D]
            values[r, cols] = parts[2 * g + half, :, D : 2 * D]


def unpack(parts):
    vmem = pl.BlockSpec(memory_space=pltpu.VMEM)
    return pl.pallas_call(
        unpack_kernel,
        in_specs=[vmem],
        out_specs=[vmem, vmem],
        out_shape=[jax.ShapeDtypeStruct((32, 8 * D), jnp.float32)] * 2,
        compiler_params=pltpu.CompilerParams(vmem_limit_bytes=4 * 1024 * 1024),
        name="unpack",
    )(parts)


def pack(keys, values):
    hbm = pl.BlockSpec(memory_space=pltpu.HBM)
    return pl.pallas_call(
        pack_kernel,
        in_specs=[hbm, hbm],
        out_specs=pl.BlockSpec(memory_space=pltpu.VMEM),
        scratch_shapes=[
            pltpu.VMEM(keys.shape, keys.dtype),
            pltpu.VMEM(values.shape, values.dtype),
            pltpu.SemaphoreType.DMA,
        ],
        out_shape=jax.ShapeDtypeStruct((16, 16, 2 * D), jnp.bfloat16),
        compiler_params=pltpu.CompilerParams(vmem_limit_bytes=4 * 1024 * 1024),
        name="pack",
    )(keys, values)


SWAP = [(0, 1), (1, 0)]


def turn(k):
    return [(i, (i + k) % NZ) for i in range(NZ)]


def body(
    queries, keys, values, attn_out, out_grad, log_norm, block_layout, document_ids, block_order
):
    z = lax.axis_index("z")
    c = lax.axis_index("c")
    p = lax.axis_index("p")
    meta = jnp.stack([z, c, p]).astype(jnp.int32)

    kv = pack(keys, values)
    kv = lax.all_to_all(kv, HEAD, 0, 0, tiled=True).reshape(CHUNK, 2 * D)
    kvs = {0: kv}
    for kk in INS:
        kvs[kk] = lax.ppermute(kv, "z", turn(kk))

    qg0 = jnp.concatenate([queries, out_grad], axis=1)
    qg2 = lax.ppermute(qg0, "p", SWAP)
    qg1 = lax.ppermute(qg0, "c", SWAP)
    qg3 = lax.ppermute(qg2, "c", SWAP)
    delta = jnp.sum(
        (out_grad.astype(jnp.float32) * attn_out.astype(jnp.float32)).reshape(512, 2, D), axis=2
    ).T
    aux0 = jnp.concatenate([log_norm, delta], axis=0)
    aux2 = lax.ppermute(aux0, "p", SWAP)
    aux1 = lax.ppermute(aux0, "c", SWAP)
    aux3 = lax.ppermute(aux2, "c", SWAP)
    code0 = block_layout[0] + 2 * block_layout[1]
    code2 = lax.ppermute(code0, "p", SWAP)
    code = code0 + 4 * code2
    docs = jnp.arange(DOCS, dtype=jnp.int32)
    sd = jnp.sum((document_ids[None, :] < docs[:, None]).astype(jnp.int32), axis=1)

    common = (block_order, sd, code, meta, (aux0, aux1, aux2, aux3))
    pooled = (queries, out_grad, qg1, qg2, qg3)
    dq, own, *parts, qs, gs = attend(FIRST, True, *common, [kvs[kk] for kk in FIRST], pooled)
    back = {}
    for kk, part in zip(FIRST[1:], parts):
        back[kk] = lax.ppermute(part, "z", turn(-kk))
    dq, *parts = attend(SECOND, False, *common, [kvs[kk] for kk in SECOND], (qs, gs, dq))
    other = lax.ppermute(dq[4:], "c", SWAP)
    high = (dq[:4, :, 2 * BLOCK :] + other[:, :, 2 * BLOCK :]).astype(jnp.bfloat16)
    parts[-1], high = lax.optimization_barrier((parts[-1], high))
    for kk, part in zip(SECOND, parts):
        back[kk] = lax.ppermute(part, "z", turn(-kk))
    mate = lax.ppermute(high, "p", SWAP)
    query_grad = flip(dq, other, mate)

    total = own
    for kk in INS:
        total = total + back[kk].astype(jnp.float32)
    out = lax.all_to_all(total.reshape(16, 16, 2 * D), HEAD, 0, 0, tiled=True)
    key_grad, value_grad = unpack(out)
    return query_grad, key_grad, value_grad


def solution(mesh):
    fine = Mesh(mesh.devices.reshape(NZ, 2, 4, 2, 2), ("z", "c") + HEAD)
    seq = ("z", "c")
    in_specs = (
        P(seq, HEAD),
        P(seq + HEAD, None),
        P(seq + HEAD, None),
        P(seq, HEAD),
        P(seq, HEAD),
        P(HEAD, seq),
        P(HEAD, None, None),
        P(),
        P(),
    )
    out_specs = (P(seq, HEAD), P(seq + HEAD, None), P(seq + HEAD, None))

    return jax.shard_map(body, mesh=fine, in_specs=in_specs, out_specs=out_specs, check_vma=False)
```

```python
import math

import jax
import jax.numpy as jnp
from jax import lax
from jax.experimental import pallas as pl
from jax.experimental.pallas import tpu as pltpu
from jax.sharding import Mesh, PartitionSpec as P

D = 128
BLOCK = 128
HALF = 64
CHUNK = 4 * HALF
SCALE = D ** (-0.5)
LOG2E = math.log2(math.e)
NZ = 8
NQ = 8
ROWS = 4 * BLOCK
DOCS = 8
UNROLL = 3
FIRST = (0, 4, 3, 5)
SECOND = (2, 6, 1, 7)
INS = FIRST[1:] + SECOND

HEAD = ("x", "w", "p")


def make_kernel(offsets, first):
    nc = len(offsets)
    nk = 4 * nc

    def kernel(bo, sd, code, meta, *refs):
        if first:
            q0, g0, qg1, qg2, qg3 = refs[:5]
            refs = refs[5:]
        else:
            qs, gs, dq_in = refs[:3]
            refs = refs[3:]
        a0, a1, a2, a3 = refs[:4]
        refs = refs[4:]
        kvs, refs = refs[:nc], refs[nc:]
        dqt, refs = refs[0], refs[1:]
        outs, refs = refs[:nc], refs[nc:]
        if first:
            qs, gs, refs = refs[0], refs[1], refs[2:]
        rows, spans, kv, acc, pt, dst, kvt, tags, lst, sem = refs
        z, c, p = meta[0], meta[1], meta[2]

        copies = []
        for dc in range(2):
            for dp in range(2):
                aux = ((a0, a2), (a1, a3))[dc][dp]
                for b in range(4):
                    i = dc * 4 + b
                    r = pl.ds(b * BLOCK, BLOCK)
                    for j in range(2):
                        h = dp * 2 + j
                        hr = pl.ds(h * BLOCK, BLOCK)
                        srcs = ()
                        if first and dc == 0 and dp == 0:
                            srcs = ((q0, 0, qs), (g0, 0, gs))
                        elif first:
                            sq = {(1, 0): qg1, (0, 1): qg2, (1, 1): qg3}[(dc, dp)]
                            srcs = ((sq, 0, qs), (sq, 2 * D, gs))
                        for src, o, dest in srcs:
                            cp = pltpu.make_async_copy(
                                src.at[r, pl.ds(o + j * D, D)], dest.at[i, hr, :], sem
                            )
                            cp.start()
                            copies.append(cp)
                        rs = slice(b * BLOCK, (b + 1) * BLOCK)
                        hs = slice(h * BLOCK, (h + 1) * BLOCK)
                        rows[i, 0:1, hs] = aux[j : j + 1, rs] * LOG2E
                        rows[i, 1:2, hs] = aux[2 + j : 3 + j, rs]
        for n, k in enumerate(offsets):
            kv[n * CHUNK : (n + 1) * CHUNK, :] = kvs[n][...]
            zk = lax.rem(z - k + NZ, NZ)
            for b in range(4):
                hb = n * 4 + b
                tags[hb] = hb + (bo[4 * (2 * zk + c) + b] << 8)
        acc[...] = jnp.zeros_like(acc)
        if first:
            dqt[...] = jnp.zeros_like(dqt)
        else:
            dqt[...] = dq_in[...]

        sub = lax.broadcasted_iota(jnp.int32, (HALF, BLOCK), 0)
        offs = (sub // 16) * 32 + 16 * p + sub % 16
        lane = lax.broadcasted_iota(jnp.int32, (1, BLOCK), 1)

        def scan(i, n):
            cq = jnp.where(i < 4, c, 1 - c)
            bq = bo[4 * (2 * z + cq) + (i & 3)]
            head = bq * BLOCK
            start0 = jnp.int32(0)
            pos_row = lane + head
            start_row = jnp.zeros_like(pos_row)
            for d in range(DOCS):
                s = sd[d]
                start0 = jnp.where(s <= head, jnp.maximum(start0, s), start0)
                start_row = jnp.where(s <= pos_row, jnp.maximum(start_row, s), start_row)
            spans[i, 0:1, :] = pos_row
            spans[i, 1:2, :] = start_row
            b0 = start0 // BLOCK
            mark = i << 20
            for hb in range(nk):
                tag = tags[hb]
                bk = tag >> 8
                cd = code[bq, bk]
                act = (bk <= bq) & (bk >= b0) & (cd != 0)
                lst[n] = tag + (cd << 16) + mark
                n = n + act.astype(jnp.int32)
            for e in range(3):
                lst[n + e] = mark
            return (n + 3) & -4

        n = lax.fori_loop(0, NQ, scan, jnp.int32(0))
        for e in range(4 * (UNROLL - 1)):
            lst[n + e] = 0
        for cp in copies:
            cp.wait()

        def tile(t, u):
            hbs, bases, bits = [], [], []
            i = lst[4 * t] >> 20
            for m in range(4):
                word = lst[4 * t + m]
                hb = pl.multiple_of((word & 255) * HALF, HALF)
                hbs.append(hb)
                bases.append(((word >> 8) & 255) * BLOCK)
                bits.append(word >> 16)
                kvt[u, m * HALF : (m + 1) * HALF, :] = kv[pl.ds(hb, HALF), :]
            keys = kvt[u, :, 0:D]
            vals = kvt[u, :, D : 2 * D]
            pos_row = spans[i, 0:1, :]
            start_row = spans[i, 1:2, :]
            nt = (((1,), (1,)), ((), ()))
            st = lax.dot_general(keys, qs[i], nt, preferred_element_type=jnp.float32)
            dpt = lax.dot_general(vals, gs[i], nt, preferred_element_type=jnp.float32)
            for h in range(4):
                hc = slice(h * BLOCK, (h + 1) * BLOCK)
                lse = rows[i, 0:1, hc]
                delta = rows[i, 1:2, hc]
                for m in range(4):
                    mr = slice(m * HALF, (m + 1) * HALF)
                    up = jnp.where((bits[m] >> h) & 1 == 1, pos_row - bases[m], -1)
                    lo = start_row - bases[m]
                    mask = (offs <= up) & (offs >= lo)
                    w = jnp.where(mask, jnp.exp2(st[mr, hc] * (SCALE * LOG2E) - lse), 0.0)
                    pt[u, mr, hc] = w.astype(jnp.bfloat16)
                    dst[u, mr, hc] = (w * (dpt[mr, hc] - delta)).astype(jnp.bfloat16)
            nn = (((1,), (0,)), ((), ()))
            dk = lax.dot_general(dst[u], qs[i], nn, preferred_element_type=jnp.float32)
            dv = lax.dot_general(pt[u], gs[i], nn, preferred_element_type=jnp.float32)
            dq = lax.dot_general(
                keys, dst[u], (((0,), (0,)), ((), ())), preferred_element_type=jnp.float32
            )
            return i, hbs, dk, dv, dq

        def tiles(t, _):
            done = [tile(UNROLL * t + u, u) for u in range(UNROLL)]
            for i, hbs, dk, dv, dq in done:
                dqt[i] += dq
                for m in range(4):
                    mr = slice(m * HALF, (m + 1) * HALF)
                    acc[pl.ds(hbs[m], HALF), 0:D] += dk[mr, :]
                    acc[pl.ds(hbs[m], HALF), D : 2 * D] += dv[mr, :]
            return 0

        lax.fori_loop(0, (n // 4 + UNROLL - 1) // UNROLL, tiles, 0)

        for n in range(nc):
            cr = slice(n * CHUNK, (n + 1) * CHUNK)
            dest = outs[n]
            dest[:, 0:D] = (acc[cr, 0:D] * SCALE).astype(dest.dtype)
            dest[:, D : 2 * D] = acc[cr, D : 2 * D].astype(dest.dtype)

    return kernel


def attend(offsets, first, bo, sd, code, meta, aux, kvs, before):
    nc = len(offsets)
    smem = pl.BlockSpec(memory_space=pltpu.SMEM)
    vmem = pl.BlockSpec(memory_space=pltpu.VMEM)
    hbm = pl.BlockSpec(memory_space=pltpu.HBM)
    shapes = [jax.ShapeDtypeStruct((NQ, D, ROWS), jnp.float32)] + [
        jax.ShapeDtypeStruct((CHUNK, 2 * D), jnp.bfloat16 if k else jnp.float32) for k in offsets
    ]
    if first:
        shapes += [jax.ShapeDtypeStruct((NQ, ROWS, D), jnp.bfloat16)] * 2
    return pl.pallas_call(
        make_kernel(offsets, first),
        in_specs=[smem] * 4 + [hbm if first else vmem] * len(before) + [vmem] * (4 + nc),
        out_specs=[vmem] * len(shapes),
        out_shape=shapes,
        scratch_shapes=[
            pltpu.VMEM((NQ, 8, ROWS), jnp.float32),
            pltpu.VMEM((NQ, 8, BLOCK), jnp.int32),
            pltpu.VMEM((nc * CHUNK, 2 * D), jnp.bfloat16),
            pltpu.VMEM((nc * CHUNK, 2 * D), jnp.float32),
            pltpu.VMEM((UNROLL, CHUNK, ROWS), jnp.bfloat16),
            pltpu.VMEM((UNROLL, CHUNK, ROWS), jnp.bfloat16),
            pltpu.VMEM((UNROLL, CHUNK, 2 * D), jnp.bfloat16),
            pltpu.SMEM((4 * nc,), jnp.int32),
            pltpu.SMEM((NQ * 4 * nc + 4 * UNROLL + 4,), jnp.int32),
            pltpu.SemaphoreType.DMA,
        ],
        compiler_params=pltpu.CompilerParams(vmem_limit_bytes=16 * 1024 * 1024),
        name="attend_first" if first else "attend_second",
    )(bo, sd, code, meta, *before, *aux, *kvs)


def pack_kernel(keys_in, values_in, out, keys, values, sem):
    copies = [pltpu.make_async_copy(keys_in, keys, sem), pltpu.make_async_copy(values_in, values, sem)]
    for cp in copies:
        cp.start()
    for cp in copies:
        cp.wait()
    for g in range(8):
        for half in range(2):
            r, cols = slice(16 * half, 16 * half + 16), slice(g * D, (g + 1) * D)
            out[2 * g + half, :, 0:D] = keys[r, cols]
            out[2 * g + half, :, D : 2 * D] = values[r, cols]


def flip_kernel(dq, other, mate, out):
    for b in range(4):
        for j in range(2):
            cols = slice(j * BLOCK, (j + 1) * BLOCK)
            part = dq[b, :, cols] + other[b, :, cols] + mate[b, :, cols].astype(jnp.float32)
            out[b * BLOCK : (b + 1) * BLOCK, j * D : (j + 1) * D] = part.T * SCALE


def flip(dq, other, mate):
    half = pl.BlockSpec((4, D, 2 * BLOCK), lambda i: (0, 0, 0))
    return pl.pallas_call(
        flip_kernel,
        grid=(1,),
        in_specs=[half] * 3,
        out_specs=pl.BlockSpec((4 * BLOCK, 2 * D), lambda i: (0, 0)),
        out_shape=jax.ShapeDtypeStruct((4 * BLOCK, 2 * D), jnp.float32),
        compiler_params=pltpu.CompilerParams(vmem_limit_bytes=8 * 1024 * 1024),
        name="flip",
    )(dq, other, mate)


def unpack_kernel(parts, keys, values):
    for g in range(8):
        for half in range(2):
            r, cols = slice(16 * half, 16 * half + 16), slice(g * D, (g + 1) * D)
            keys[r, cols] = parts[2 * g + half, :, 0:D].astype(jnp.float32)
            values[r, cols] = parts[2 * g + half, :, D : 2 * D].astype(jnp.float32)


def unpack(parts):
    vmem = pl.BlockSpec(memory_space=pltpu.VMEM)
    return pl.pallas_call(
        unpack_kernel,
        in_specs=[vmem],
        out_specs=[vmem, vmem],
        out_shape=[jax.ShapeDtypeStruct((32, 8 * D), jnp.float32)] * 2,
        compiler_params=pltpu.CompilerParams(vmem_limit_bytes=4 * 1024 * 1024),
        name="unpack",
    )(parts)


def pack(keys, values):
    hbm = pl.BlockSpec(memory_space=pltpu.HBM)
    return pl.pallas_call(
        pack_kernel,
        in_specs=[hbm, hbm],
        out_specs=pl.BlockSpec(memory_space=pltpu.VMEM),
        scratch_shapes=[
            pltpu.VMEM(keys.shape, keys.dtype),
            pltpu.VMEM(values.shape, values.dtype),
            pltpu.SemaphoreType.DMA,
        ],
        out_shape=jax.ShapeDtypeStruct((16, 16, 2 * D), jnp.bfloat16),
        compiler_params=pltpu.CompilerParams(vmem_limit_bytes=4 * 1024 * 1024),
        name="pack",
    )(keys, values)


SWAP = [(0, 1), (1, 0)]


def turn(k):
    return [(i, (i + k) % NZ) for i in range(NZ)]


def body(
    queries, keys, values, attn_out, out_grad, log_norm, block_layout, document_ids, block_order
):
    z = lax.axis_index("z")
    c = lax.axis_index("c")
    p = lax.axis_index("p")
    meta = jnp.stack([z, c, p]).astype(jnp.int32)

    kv = pack(keys, values)
    kv = lax.all_to_all(kv, HEAD, 0, 0, tiled=True).reshape(CHUNK, 2 * D)
    kvs = {0: kv}
    for kk in INS:
        kvs[kk] = lax.ppermute(kv, "z", turn(kk))

    qg0 = jnp.concatenate([queries, out_grad], axis=1)
    qg2 = lax.ppermute(qg0, "p", SWAP)
    qg1 = lax.ppermute(qg0, "c", SWAP)
    qg3 = lax.ppermute(qg2, "c", SWAP)
    delta = jnp.sum(
        (out_grad.astype(jnp.float32) * attn_out.astype(jnp.float32)).reshape(512, 2, D), axis=2
    ).T
    aux0 = jnp.concatenate([log_norm, delta], axis=0)
    aux2 = lax.ppermute(aux0, "p", SWAP)
    aux1 = lax.ppermute(aux0, "c", SWAP)
    aux3 = lax.ppermute(aux2, "c", SWAP)
    code0 = block_layout[0] + 2 * block_layout[1]
    code2 = lax.ppermute(code0, "p", SWAP)
    code = code0 + 4 * code2
    docs = jnp.arange(DOCS, dtype=jnp.int32)
    sd = jnp.sum((document_ids[None, :] < docs[:, None]).astype(jnp.int32), axis=1)

    common = (block_order, sd, code, meta, (aux0, aux1, aux2, aux3))
    pooled = (queries, out_grad, qg1, qg2, qg3)
    dq, own, *parts, qs, gs = attend(FIRST, True, *common, [kvs[kk] for kk in FIRST], pooled)
    back = {}
    for kk, part in zip(FIRST[1:], parts):
        back[kk] = lax.ppermute(part, "z", turn(-kk))
    dq, *parts = attend(SECOND, False, *common, [kvs[kk] for kk in SECOND], (qs, gs, dq))
    other = lax.ppermute(dq[4:], "c", SWAP)
    high = (dq[:4, :, 2 * BLOCK :] + other[:, :, 2 * BLOCK :]).astype(jnp.bfloat16)
    parts[-1], high = lax.optimization_barrier((parts[-1], high))
    for kk, part in zip(SECOND, parts):
        back[kk] = lax.ppermute(part, "z", turn(-kk))
    mate = lax.ppermute(high, "p", SWAP)
    query_grad = flip(dq, other, mate)

    total = own
    for kk in INS:
        total = total + back[kk].astype(jnp.float32)
    out = lax.all_to_all(total.astype(jnp.bfloat16).reshape(16, 16, 2 * D), HEAD, 0, 0, tiled=True)
    key_grad, value_grad = unpack(out)
    return query_grad, key_grad, value_grad


def solution(mesh):
    fine = Mesh(mesh.devices.reshape(NZ, 2, 4, 2, 2), ("z", "c") + HEAD)
    seq = ("z", "c")
    in_specs = (
        P(seq, HEAD),
        P(seq + HEAD, None),
        P(seq + HEAD, None),
        P(seq, HEAD),
        P(seq, HEAD),
        P(HEAD, seq),
        P(HEAD, None, None),
        P(),
        P(),
    )
    out_specs = (P(seq, HEAD), P(seq + HEAD, None), P(seq + HEAD, None))

    return jax.shard_map(body, mesh=fine, in_specs=in_specs, out_specs=out_specs, check_vma=False)
```
